32 devices in a mesh: frames: 4 (over z), states: 8 (over y, x, core).
Axes of the slice: x: 2, y: 2, z: 4, core: 2. Of those that a mesh axis runs over, the one named last changes fastest.
Arguments:
- features: bfloat16 [2048, 1024], P('states', 'frames'), may hold values from -10 to 10
- state_ids: int32 [2048, 32], P('states'), may hold values from 0 to 767, as said below
- weights: float32 [2048, 32], P('states'), may hold values from 0.05 to 1
Outputs:
- means: bfloat16 [768, 1024], P(None, 'frames')
- precisions: bfloat16 [768, 1024], P(None, 'frames')
- frame_score: float32 [2048], P('states')
The draws below stay inside these ranges and needn't reach their ends.
Inputs may be any that keep to these rules, and one draw needn't show every extreme that they name: `state_ids`: each row names 32 different states; every state is named by some row.
All inputs are finite; a program needn't handle non-finite values.
Results may differ from the reference program's by a relative error of at most 0.0034.
Values may be sent and summed in bfloat16 or wider, within the bound.
No kernel may reach another device: no remote copies, remote signals or barrier semaphores. Data moves between devices by JAX's collectives and lax.ppermute only.
A program may use at most 128 MiB of HBM per device.

```python
import math
import jax
import jax.numpy as jnp
from jax import lax

D = 1024
TOPK = 32
ALL_STATES = 768
ALL_FRAMES = 2048


def frame_layout(key):
    base_key = jax.random.fold_in(key, 101)
    layout_keys = jax.random.split(base_key, 6)
    cluster_count = ALL_STATES // (2 * TOPK)
    order = jax.random.permutation(layout_keys[0], ALL_FRAMES).astype(jnp.int32)
    home = order % cluster_count
    rank = order // cluster_count
    return (home, rank, layout_keys)


def draw_state_ids(key, part):
    home, rank, layout_keys = frame_layout(key)
    group = 2 * TOPK
    cluster_count = ALL_STATES // group
    outside = TOPK // 8
    inside = TOPK - outside
    state_order = jax.random.permutation(layout_keys[1], ALL_STATES).astype(jnp.int32)
    position = jnp.arange(group, dtype=jnp.int32)[None, :]
    random_score = jax.random.randint(layout_keys[2], (ALL_FRAMES, group), 0, 2 ** 20, dtype=jnp.int32) * group + position
    forced_score = (position - rank[:, None] * inside) % group
    score = jnp.where(rank[:, None] < 3, forced_score, random_score)
    picked = jnp.argsort(score, axis=1)[:, :inside].astype(jnp.int32)
    chosen = home[:, None] * group + picked
    if outside > 0:
        offset = jax.random.randint(layout_keys[3], (ALL_FRAMES,), 1, cluster_count, dtype=jnp.int32)
        neighbour = (home + offset) % cluster_count
        other_score = jax.random.randint(layout_keys[4], (ALL_FRAMES, group), 0, 2 ** 20, dtype=jnp.int32) * group + position
        extra = jnp.argsort(other_score, axis=1)[:, :outside].astype(jnp.int32)
        chosen = jnp.concatenate([chosen, neighbour[:, None] * group + extra], axis=1)
    state_list = state_order[chosen]
    column_score = jax.random.randint(layout_keys[5], (ALL_FRAMES, TOPK), 0, 2 ** 20, dtype=jnp.int32) * TOPK + jnp.arange(TOPK, dtype=jnp.int32)[None, :]
    column_order = jnp.argsort(column_score, axis=1).astype(jnp.int32)
    return jnp.take_along_axis(state_list, column_order, axis=1).astype(jnp.int32)


def draw_features(key, part):
    home, rank, layout_keys = frame_layout(key)
    cluster_count = ALL_STATES // (2 * TOPK)
    feature_keys = jax.random.split(jax.random.fold_in(key, 17), 5)
    scales = jnp.exp(jax.random.uniform(feature_keys[0], (D,), jnp.float32, math.log(0.2), math.log(2.0)))
    offsets = jax.random.uniform(feature_keys[1], (D,), jnp.float32, -1.5, 1.5)
    cluster_shift = jax.random.uniform(feature_keys[3], (cluster_count, D), jnp.float32, -1.0, 1.0)
    cluster_scale = jnp.exp(jax.random.uniform(feature_keys[4], (cluster_count,), jnp.float32, math.log(0.5), math.log(2.0)))
    noise = jnp.clip(jax.random.normal(feature_keys[2], (ALL_FRAMES, D), jnp.float32), -4.0, 4.0)
    centre = offsets[None, :] + 1.5 * cluster_shift[home]
    spread = scales[None, :] * cluster_scale[home][:, None]
    return jnp.clip(centre + spread * noise, -10.0, 10.0).astype(jnp.bfloat16)


def level_of(stream_key, extent, cuts, low, largest):
    def one(dim, blocks):
        heights = jax.random.uniform(jax.random.fold_in(jax.random.fold_in(stream_key, 6), dim), (blocks,), jnp.float32, low / len(cuts), largest / len(cuts))
        return jnp.repeat(jnp.exp(heights), extent[dim] // blocks).reshape((-1,) + (1,) * (len(extent) - dim - 1))

    gain = one(*cuts[0])
    for cut in cuts[1:]:
        gain = gain * one(*cut)
    return gain


def setup_inputs(seed: int = 0) -> dict:
    key_of = jax.random.split(jax.random.key(seed), 4)
    features = draw_features(jax.random.fold_in(key_of[3], 71), 0)
    state_ids = draw_state_ids(jax.random.fold_in(key_of[3], 71), 0)
    weights = jnp.clip(jnp.exp(math.log(1.0) - 2.9957323 * jax.random.uniform(key_of[2], (ALL_FRAMES, TOPK), jnp.float32) ** level_of(key_of[2], (ALL_FRAMES, TOPK), ((0, 8),), -0.2, 0.2)), 0.05, 1.0)
    return dict(features=features, state_ids=state_ids, weights=weights)


variance_floor = 0.25


def reference(features, state_ids, weights):
    rounded = lax.optimization_barrier(weights.astype(jnp.bfloat16)).astype(jnp.float32)
    values = features.astype(jnp.float32)
    squares = lax.optimization_barrier((values * values).astype(jnp.bfloat16)).astype(jnp.float32)
    first = jnp.zeros((ALL_STATES, D), jnp.float32)
    second = jnp.zeros((ALL_STATES, D), jnp.float32)
    occupancy = jnp.zeros((ALL_STATES,), jnp.float32)
    for column in range(TOPK):
        chosen = state_ids[:, column]
        weight_col = rounded[:, column]
        first = first.at[chosen].add(weight_col[:, None] * values)
        second = second.at[chosen].add(weight_col[:, None] * squares)
        occupancy = occupancy.at[chosen].add(weight_col)
    mean_value = first / occupancy[:, None]
    variance = jnp.maximum(second / occupancy[:, None] - mean_value * mean_value, variance_floor)
    means = mean_value.astype(jnp.bfloat16)
    precisions = (1.0 / variance).astype(jnp.bfloat16)
    mean_f = means.astype(jnp.float32)
    prec_f = precisions.astype(jnp.float32)
    product = lax.optimization_barrier((mean_f * prec_f).astype(jnp.bfloat16)).astype(jnp.float32)
    constant = jnp.sum(mean_f * product - jnp.log(prec_f), axis=1)
    quadratic = jnp.zeros((ALL_FRAMES,), jnp.float32)
    for column in range(TOPK):
        chosen = state_ids[:, column]
        likely = jnp.sum(squares * prec_f[chosen] - 2.0 * values * product[chosen], axis=1) + constant[chosen]
        quadratic = quadratic + rounded[:, column] * likely
    frame_score = -0.5 * quadratic / (D * jnp.sum(rounded, axis=1))
    return means, precisions, frame_score
```

```python
import functools
import jax
import jax.numpy as jnp
from jax import lax
from jax.experimental import pallas as pl
from jax.experimental.pallas import tpu as pltpu
from jax.sharding import PartitionSpec as P

STATE_DEV = 96
GROUP = 128
variance_floor = 0.25


def encode(ids):
    return ((GROUP + (ids & (GROUP - 1))) << (ids // GROUP)).astype(jnp.float32).astype(jnp.bfloat16)


def vmem(n):
    return [pl.BlockSpec(memory_space=pltpu.VMEM)] * n


def build_kernel(count, topk, *refs):
    params, (post_ref, occ_ref) = refs[:count], refs[count:]
    states = post_ref.shape[0]
    frames = params[0].shape[1]
    base = (lax.broadcasted_iota(jnp.int32, (GROUP, 128), 0) + GROUP).astype(jnp.float32)
    for chunk, ref in enumerate(params):
        for tile in range(frames // 128):
            lanes = slice(tile * 128, tile * 128 + 128)
            wts = ref[:topk, lanes]
            codes = ref[topk:, lanes]
            for group in range(states // GROUP):
                rows = slice(group * GROUP, (group + 1) * GROUP)
                names = (base * float(2 ** group)).astype(jnp.bfloat16)
                acc = jnp.zeros((GROUP, 128), jnp.bfloat16)
                for j in range(topk):
                    acc = jnp.where(codes[j : j + 1] == names, wts[j : j + 1], acc)
                post_ref[rows, chunk * frames + tile * 128 : chunk * frames + tile * 128 + 128] = acc
                part = acc.astype(jnp.float32)
                if chunk == 0 and tile == 0:
                    occ_ref[rows, :] = part
                else:
                    occ_ref[rows, :] += part


def build(params, states):
    topk, frames = params[0].shape[0] // 2, params[0].shape[1]
    n = len(params)
    return pl.pallas_call(
        functools.partial(build_kernel, n, topk),
        out_shape=(
            jax.ShapeDtypeStruct((states, n * frames), jnp.bfloat16),
            jax.ShapeDtypeStruct((states, 128), jnp.float32),
        ),
        in_specs=vmem(n),
        out_specs=tuple(vmem(2)),
        compiler_params=pltpu.CompilerParams(vmem_limit_bytes=16 << 20),
        cost_estimate=pl.CostEstimate(flops=states * frames * n * 8000, bytes_accessed=1 << 20, transcendentals=0),
        name="build%d" % n,
    )(*params)


def fill(pair_ref, feats):
    width = feats[0].shape[1]
    rows = feats[0].shape[0]
    for i, ref in enumerate(feats):
        x = ref[...]
        xf = x.astype(jnp.float32)
        pair_ref[i * rows : (i + 1) * rows, :width] = x
        pair_ref[i * rows : (i + 1) * rows, width:] = (xf * xf).astype(jnp.bfloat16)


def sums_kernel(nf, npost, *refs):
    feats, posts, (out_ref, pair_ref) = refs[:nf], refs[nf : nf + npost], refs[nf + npost :]
    fill(pair_ref, feats)
    at = 0
    total = None
    for ref in posts:
        k = ref.shape[1]
        part = jnp.dot(ref[...], pair_ref[at : at + k, :], preferred_element_type=jnp.float32)
        total = part if total is None else total + part
        at += k
    out_ref[...] = total


def sums(feats, posts):
    rows, width = feats[0].shape
    states = posts[0].shape[0]
    nf, npost = len(feats), len(posts)
    return pl.pallas_call(
        functools.partial(sums_kernel, nf, npost),
        out_shape=jax.ShapeDtypeStruct((states, 2 * width), jnp.float32),
        in_specs=vmem(nf + npost),
        out_specs=vmem(1)[0],
        scratch_shapes=[pltpu.VMEM((nf * rows, 2 * width), jnp.bfloat16)],
        compiler_params=pltpu.CompilerParams(vmem_limit_bytes=16 << 20),
        cost_estimate=pl.CostEstimate(flops=2 * states * nf * rows * 2 * width, bytes_accessed=4 << 20, transcendentals=0),
        name="sums",
    )(*feats, *posts)


def final_kernel(nf, nocc, topk, full_width, *refs):
    feats = refs[:nf]
    own_ref, par_ref, own_post_ref, post_ref, partial_ref = refs[nf : nf + 5]
    occs = refs[nf + 5 : nf + 5 + nocc]
    mean_out, prec_out, score_ref, pair_ref, mean_ref, prec_ref, table_ref, sem = refs[nf + 5 + nocc :]
    rows, width = own_ref.shape
    fill(pair_ref, feats)
    total = partial_ref[...] + jnp.dot(post_ref[...], pair_ref[...], preferred_element_type=jnp.float32)
    occ = occs[0][...]
    for ref in occs[1:]:
        occ = occ + ref[...]
    inverse = 1.0 / jnp.sum(occ, axis=1, keepdims=True)
    mean = total[:, :width] * inverse
    variance = jnp.maximum(total[:, width:] * inverse - mean * mean, variance_floor)
    means = mean.astype(jnp.bfloat16)
    precs = (1.0 / variance).astype(jnp.bfloat16)
    mean_ref[...] = means
    prec_ref[...] = precs
    copies = [
        pltpu.make_async_copy(mean_ref, mean_out, sem.at[0]),
        pltpu.make_async_copy(prec_ref, prec_out, sem.at[1]),
    ]
    for copy in copies:
        copy.start()
    mean_f = means.astype(jnp.float32)
    prec_f = precs.astype(jnp.float32)
    product = (mean_f * prec_f).astype(jnp.bfloat16).astype(jnp.float32)
    constant = jnp.sum(mean_f * product - jnp.log(prec_f), axis=1, keepdims=True)
    table_ref[:, :width] = (-2.0 * product).astype(jnp.bfloat16)
    table_ref[:, width:] = precs
    own = own_ref[...]
    own_f = own.astype(jnp.float32)
    both = jnp.concatenate([own, (own_f * own_f).astype(jnp.bfloat16)], axis=1)
    likely = lax.dot_general(table_ref[...], both, (((1,), (1,)), ((), ())), preferred_element_type=jnp.float32)
    quad = jnp.sum((likely + constant) * own_post_ref[:, :rows].astype(jnp.float32), axis=0, keepdims=True)
    wsum = jnp.sum(par_ref[:topk, :].astype(jnp.float32), axis=0, keepdims=True)
    score_ref[...] = -0.5 * quad / (full_width * wsum)
    for copy in copies:
        copy.wait()


def final(feats, own, par, own_post, post, partial, occs, full_width):
    rows, width = own.shape
    states = post.shape[0]
    nf, nocc = len(feats), len(occs)
    hbm = pl.BlockSpec(memory_space=pl.ANY)
    out = jax.ShapeDtypeStruct((states, width), jnp.bfloat16)
    return pl.pallas_call(
        functools.partial(final_kernel, nf, nocc, par.shape[0] // 2, float(full_width)),
        out_shape=(out, out, jax.ShapeDtypeStruct((1, rows), jnp.float32)),
        in_specs=vmem(nf + 5 + nocc),
        out_specs=(hbm, hbm, vmem(1)[0]),
        scratch_shapes=[
            pltpu.VMEM((nf * rows, 2 * width), jnp.bfloat16),
            pltpu.VMEM((states, width), jnp.bfloat16),
            pltpu.VMEM((states, width), jnp.bfloat16),
            pltpu.VMEM((states, 2 * width), jnp.bfloat16),
            pltpu.SemaphoreType.DMA((2,)),
        ],
        compiler_params=pltpu.CompilerParams(vmem_limit_bytes=24 << 20),
        cost_estimate=pl.CostEstimate(flops=4 * states * rows * 4 * width, bytes_accessed=4 << 20, transcendentals=0),
        name="final",
    )(*feats, own, par, own_post, post, partial, *occs)


def swap(value, axis, k):
    n = lax.axis_size(axis)
    return lax.ppermute(value, axis, [(i, i ^ k) for i in range(n)])


def small_group(features, state_ids, weights):
    rows, width = features.shape
    group = lax.axis_size("states")
    states = STATE_DEV * group
    par = jnp.concatenate([weights.T.astype(jnp.bfloat16), encode(state_ids.T)], axis=0)
    far = [k for k in reversed(range(2, group)) if k % 2 == 0]
    par_far = [swap(par, "states", k) for k in far]
    par_near = swap(par, "states", 1)
    feat_far = [swap(features, "states", k) for k in far]
    feat_near = swap(features, "states", 1)
    post_a, occ_a = build([par, par_near], states)
    par_back = [swap(v, "states", 1) for v in par_far]
    post_b, occ_b = build(par_far, states)
    post_c, occ_c = build(par_back, states)
    feat_back = [swap(v, "states", 1) for v in feat_far]
    partial = sums([features, feat_near] + feat_far, [post_a, post_b])
    means, precisions, score = final(
        feat_back, features, par, post_a, post_c, partial, [occ_a, occ_b, occ_c], width * lax.axis_size("frames")
    )
    score = score.reshape(rows)
    k = 1
    while k < lax.axis_size("frames"):
        score = score + swap(score, "frames", k)
        k *= 2
    return means, precisions, score


def refresh(first, second, counts):
    mean_value = first / counts
    variance = jnp.maximum(second / counts - mean_value * mean_value, variance_floor)
    return (mean_value.astype(jnp.bfloat16), (1.0 / variance).astype(jnp.bfloat16))


def large_group(features, state_ids, weights):
    rows_here, local_width = features.shape
    group_size = lax.axis_size("states")
    full_width = local_width * lax.axis_size("frames")
    total_states = STATE_DEV * group_size
    row_index = jnp.arange(rows_here, dtype=jnp.int32)[:, None]
    rounded = weights.astype(jnp.bfloat16)
    posterior = (
        jnp.zeros((rows_here, total_states), jnp.bfloat16).at[row_index, state_ids].add(rounded)
    )
    values = features.astype(jnp.float32)
    squares = (values * values).astype(jnp.bfloat16)
    blocked = posterior.reshape(rows_here, group_size, STATE_DEV)
    routed = lax.all_to_all(blocked, "states", split_axis=1, concat_axis=0, tiled=True)
    routed = routed.reshape(rows_here * group_size, STATE_DEV)
    owned_counts = jnp.sum(routed, axis=0, dtype=jnp.float32)
    piece = lax.all_gather(features, "states", axis=0, tiled=True)
    piece_f = piece.astype(jnp.float32)
    piece_sq = (piece_f * piece_f).astype(jnp.bfloat16)
    joined = jnp.concatenate([piece, piece_sq], axis=1)
    owned_sums = lax.dot_general(
        routed, joined, (((0,), (0,)), ((), ())), preferred_element_type=jnp.float32
    )
    mean_rows, prec_rows = refresh(
        owned_sums[:, :local_width], owned_sums[:, local_width:], owned_counts[:, None]
    )
    packed = lax.all_gather(
        jnp.concatenate([mean_rows, prec_rows], axis=1), "states", axis=0, tiled=True
    )
    means = packed[:, :local_width]
    precisions = packed[:, local_width:]
    mean_f = means.astype(jnp.float32)
    prec_f = precisions.astype(jnp.float32)
    product = (mean_f * prec_f).astype(jnp.bfloat16)
    constant_term = jnp.sum(mean_f * product.astype(jnp.float32) - jnp.log(prec_f), axis=1)
    lookup_table = jnp.concatenate([precisions, product], axis=1)
    weight_f = rounded.astype(jnp.float32)
    blended = jnp.dot(posterior, lookup_table, preferred_element_type=jnp.float32)
    quadratic = jnp.sum(
        squares.astype(jnp.float32) * blended[:, :local_width]
        - 2.0 * values * blended[:, local_width:],
        axis=1,
    )
    quadratic = quadratic + jnp.sum(weight_f * constant_term[state_ids], axis=1)
    summed = lax.psum(quadratic, "frames")
    weight_sum = jnp.sum(weight_f, axis=1)
    frame_score = -0.5 * summed / (full_width * weight_sum)
    return (means, precisions, frame_score)


def solution(mesh):
    return jax.shard_map(
        small_group if mesh.shape["states"] <= 8 else large_group,
        mesh=mesh,
        in_specs=(P("states", "frames"), P("states", None), P("states", None)),
        out_specs=(P(None, "frames"), P(None, "frames"), P("states")),
        check_vma=False,
    )
```

```python
import functools
import jax
import jax.numpy as jnp
from jax import lax
from jax.experimental import pallas as pl
from jax.experimental.pallas import tpu as pltpu
from jax.sharding import PartitionSpec as P


STATE_DEV = 96
GROUP = 128
variance_floor = 0.25
FAR = (4, 2, 7)


def vmem(n):
    return [pl.BlockSpec(memory_space=pltpu.VMEM)] * n


def swap(value, axis, k):
    n = lax.axis_size(axis)
    return lax.ppermute(value, axis, [(i, i ^ k) for i in range(n)])


def core():
    return lax.axis_index("states") % 2


def prep_kernel(feat_ref, ids_ref, wts_ref, msg_ref, ids_buf, wts_buf, sem):
    rows = feat_ref.shape[0]
    topk = ids_ref.shape[0]
    copies = [
        pltpu.make_async_copy(ids_ref, ids_buf, sem.at[0]),
        pltpu.make_async_copy(wts_ref, wts_buf, sem.at[1]),
        pltpu.make_async_copy(feat_ref, msg_ref.at[:rows], sem.at[2]),
    ]
    for copy in copies:
        copy.start()
    copies[0].wait()
    ids = ids_buf[...]
    codes = (GROUP + (ids & (GROUP - 1))) << (ids >> 7)
    msg_ref[rows + topk :] = codes.astype(jnp.float32).astype(jnp.bfloat16)
    copies[1].wait()
    msg_ref[rows : rows + topk] = wts_buf[...].astype(jnp.bfloat16)
    copies[2].wait()


def prep(features, ids, weights):
    rows, width = features.shape
    topk = ids.shape[0]
    return pl.pallas_call(
        prep_kernel,
        out_shape=jax.ShapeDtypeStruct((rows + 2 * topk, width), jnp.bfloat16),
        in_specs=[pl.BlockSpec(memory_space=pltpu.HBM)] * 3,
        out_specs=vmem(1)[0],
        scratch_shapes=[
            pltpu.VMEM(ids.shape, ids.dtype),
            pltpu.VMEM(weights.shape, weights.dtype),
            pltpu.SemaphoreType.DMA((3,)),
        ],
        compiler_params=pltpu.CompilerParams(vmem_limit_bytes=4 << 20),
        name="prep",
    )(*[pltpu.with_memory_space_constraint(v, pltpu.HBM) for v in (features, ids, weights)])


def build(ref, topk, post_ref, at, occ):
    width = ref.shape[1]
    rows = ref.shape[0] - 2 * topk
    states = post_ref.shape[0]
    groups = states // GROUP
    scale = (1 << (core() * groups)).astype(jnp.float32)
    base = (lax.broadcasted_iota(jnp.int32, (GROUP, 128), 0) + GROUP).astype(jnp.float32) * scale
    for tile in range(width // 128):
        lanes = slice(tile * 128, tile * 128 + 128)
        wts = ref[rows : rows + topk, lanes]
        codes = ref[rows + topk :, lanes]
        for group in range(groups):
            names = (base * float(2 ** group)).astype(jnp.bfloat16)
            acc = jnp.zeros((GROUP, 128), jnp.bfloat16)
            for j in range(topk):
                acc = jnp.where(codes[j : j + 1] == names, wts[j : j + 1], acc)
            post_ref[group * GROUP : (group + 1) * GROUP, at + tile * 128 : at + tile * 128 + 128] = acc
            part = acc.astype(jnp.float32)
            occ[group] = part if occ[group] is None else occ[group] + part


def fill(ref, topk, pair_ref, at):
    width = ref.shape[1]
    rows = ref.shape[0] - 2 * topk
    x = ref[:rows]
    xf = x.astype(jnp.float32)
    pair_ref[at : at + rows, :width] = x
    pair_ref[at : at + rows, width:] = (xf * xf).astype(jnp.bfloat16)


def gather_sums(msgs, topk, post_ref, pair_ref, old_sum, old_occ):
    width = msgs[0].shape[1]
    rows = msgs[0].shape[0] - 2 * topk
    groups = post_ref.shape[0] // GROUP
    occ = [None] * groups
    if old_occ is not None:
        occ = [old_occ[g * GROUP : (g + 1) * GROUP] for g in range(groups)]
    for i, ref in enumerate(msgs):
        build(ref, topk, post_ref, i * width, occ)
        fill(ref, topk, pair_ref, i * rows)
    total = jnp.dot(post_ref[...], pair_ref[...], preferred_element_type=jnp.float32)
    if old_sum is not None:
        total = total + old_sum[...]
    return total, occ


def moments_kernel(n, topk, first, *refs):
    msgs, rest = refs[:n], refs[n:]
    if first:
        sum_ref, occ_ref, post_ref, pair_ref = rest
        old_sum = old_occ = None
    else:
        old_sum, old_occ, sum_ref, occ_ref, post_ref, pair_ref = rest
    total, occ = gather_sums(msgs, topk, post_ref, pair_ref, old_sum, old_occ)
    sum_ref[...] = total
    for g, part in enumerate(occ):
        occ_ref[g * GROUP : (g + 1) * GROUP] = part


def moments(msgs, topk, states, old):
    width = msgs[0].shape[1]
    rows = msgs[0].shape[0] - 2 * topk
    n = len(msgs)
    first = not old
    post = jax.ShapeDtypeStruct((states, n * width), jnp.bfloat16)
    outs = [jax.ShapeDtypeStruct((states, 2 * width), jnp.float32), jax.ShapeDtypeStruct((states, 128), jnp.float32)]
    scratch = [pltpu.VMEM((n * rows, 2 * width), jnp.bfloat16)]
    if first:
        outs.append(post)
    else:
        scratch.insert(0, pltpu.VMEM(post.shape, post.dtype))
    return pl.pallas_call(
        functools.partial(moments_kernel, n, topk, first),
        out_shape=tuple(outs),
        in_specs=vmem(n + len(old)),
        out_specs=tuple(vmem(len(outs))),
        scratch_shapes=scratch,
        compiler_params=pltpu.CompilerParams(vmem_limit_bytes=16 << 20),
        cost_estimate=pl.CostEstimate(flops=states * rows * n * 4000, bytes_accessed=1 << 20, transcendentals=0),
    )(*msgs, *old)


def final_kernel(n, topk, full_width, *refs):
    msgs = refs[:n]
    own_ref, near_ref, own_post_ref, old_sum, old_occ = refs[n : n + 5]
    half_ref, score_ref, post_ref, pair_ref, table_ref, both_ref = refs[n + 5 :]
    width = own_ref.shape[1]
    rows = own_ref.shape[0] - 2 * topk
    states = post_ref.shape[0]
    me = core()
    total, occ = gather_sums(msgs, topk, post_ref, pair_ref, old_sum, old_occ)
    occ = jnp.concatenate(occ, axis=0)
    inverse = 1.0 / jnp.sum(occ, axis=1, keepdims=True)
    mean = total[:, :width] * inverse
    variance = jnp.maximum(total[:, width:] * inverse - mean * mean, variance_floor)
    means = mean.astype(jnp.bfloat16)
    precs = (1.0 / variance).astype(jnp.bfloat16)
    half_ref[:states] = means
    half_ref[states:] = precs
    mean_f = means.astype(jnp.float32)
    prec_f = precs.astype(jnp.float32)
    product = (mean_f * prec_f).astype(jnp.bfloat16).astype(jnp.float32)
    constant = jnp.sum(mean_f * product - jnp.log(prec_f), axis=1, keepdims=True)
    table_ref[:, :width] = (-2.0 * product).astype(jnp.bfloat16)
    table_ref[:, width:] = precs
    fill(own_ref, topk, both_ref, 0)
    fill(near_ref, topk, both_ref, rows)
    likely = lax.dot_general(table_ref[...], both_ref[...], (((1,), (1,)), ((), ())), preferred_element_type=jnp.float32)
    quad = jnp.sum((likely + constant) * own_post_ref[...].astype(jnp.float32), axis=0, keepdims=True)
    for ref, row, at in ((own_ref, me, 0), (near_ref, 1 - me, rows)):
        wsum = jnp.sum(ref[rows : rows + topk].astype(jnp.float32), axis=0, keepdims=True)
        score_ref[pl.ds(row, 1)] = -0.5 * quad[:, at : at + rows] / (full_width * wsum)


def final(msgs, topk, own, near, own_post, old, full_width):
    width = own.shape[1]
    rows = own.shape[0] - 2 * topk
    states = own_post.shape[0]
    n = len(msgs)
    out = jax.ShapeDtypeStruct((2 * states, width), jnp.bfloat16)
    return pl.pallas_call(
        functools.partial(final_kernel, n, topk, float(full_width)),
        out_shape=(out, jax.ShapeDtypeStruct((2, rows), jnp.float32)),
        in_specs=vmem(n + 5),
        out_specs=tuple(vmem(2)),
        scratch_shapes=[
            pltpu.VMEM((states, n * width), jnp.bfloat16),
            pltpu.VMEM((n * rows, 2 * width), jnp.bfloat16),
            pltpu.VMEM((states, 2 * width), jnp.bfloat16),
            pltpu.VMEM((2 * rows, 2 * width), jnp.bfloat16),
        ],
        compiler_params=pltpu.CompilerParams(vmem_limit_bytes=16 << 20),
        cost_estimate=pl.CostEstimate(flops=8 * states * rows * 4 * width, bytes_accessed=4 << 20, transcendentals=0),
        name="final",
    )(*msgs, own, near, own_post, *old)


def place_kernel(mine_ref, other_ref, mean_out, prec_out, sem):
    states = mine_ref.shape[0] // 2
    copies = []
    for i, (ref, where) in enumerate(((mine_ref, core()), (other_ref, 1 - core()))):
        rows = pl.ds(pl.multiple_of(where * states, states), states)
        copies.append(pltpu.make_async_copy(ref.at[:states], mean_out.at[rows], sem.at[2 * i]))
        copies.append(pltpu.make_async_copy(ref.at[states:], prec_out.at[rows], sem.at[2 * i + 1]))
    for copy in copies:
        copy.start()
    for copy in copies:
        copy.wait()


def place(mine, other):
    hbm = pl.BlockSpec(memory_space=pltpu.HBM)
    out = jax.ShapeDtypeStruct(mine.shape, mine.dtype)
    return pl.pallas_call(
        place_kernel,
        out_shape=(out, out),
        in_specs=vmem(2),
        out_specs=(hbm, hbm),
        scratch_shapes=[pltpu.SemaphoreType.DMA((4,))],
        compiler_params=pltpu.CompilerParams(vmem_limit_bytes=4 << 20),
        cost_estimate=pl.CostEstimate(flops=1 << 20, bytes_accessed=1 << 20, transcendentals=0),
        name="place",
    )(mine, other)


def hop(value, pairs):
    return lax.ppermute(value, ("frames", "states"), pairs)


def small_group(features, state_ids, weights):
    return update(features, state_ids, weights)


def update(features, state_ids, weights):
    _, width = features.shape
    topk = state_ids.shape[1]
    group = lax.axis_size("states")
    depth = lax.axis_size("frames")
    states = STATE_DEV * group // 2
    own = prep(features, state_ids.T, weights.T)
    far = [swap(own, "states", k) for k in FAR]
    near = swap(own, "states", 1)
    back = [swap(v, "states", 1) for v in far]
    total, occ, post = moments([own, near], topk, states, ())
    old = moments([far[0]], topk, states, (total, occ))
    old = moments([back[0]], topk, states, old)
    old = moments([far[1]], topk, states, old)
    old = moments([back[1], far[2]], topk, states, old)
    half, score = final([back[2]], topk, own, near, post, old, width * depth)
    score = score + swap(score, "states", 1)
    other = swap(half, "states", 1)
    k = 1
    while k < depth:
        pairs = [(z * group + s, (z ^ k) * group + (s ^ 1)) for z in range(depth) for s in range(group)]
        score = score + hop(score, pairs)
        k *= 2
    means, precisions = place(half, other)
    return means, precisions, jnp.where(core() == 1, score[1], score[0])


def refresh(first, second, counts):
    mean_value = first / counts
    variance = jnp.maximum(second / counts - mean_value * mean_value, variance_floor)
    return (mean_value.astype(jnp.bfloat16), (1.0 / variance).astype(jnp.bfloat16))


def large_group(features, state_ids, weights):
    rows_here, local_width = features.shape
    group_size = lax.axis_size("states")
    full_width = local_width * lax.axis_size("frames")
    total_states = STATE_DEV * group_size
    row_index = jnp.arange(rows_here, dtype=jnp.int32)[:, None]
    rounded = weights.astype(jnp.bfloat16)
    posterior = (
        jnp.zeros((rows_here, total_states), jnp.bfloat16).at[row_index, state_ids].add(rounded)
    )
    values = features.astype(jnp.float32)
    squares = (values * values).astype(jnp.bfloat16)
    blocked = posterior.reshape(rows_here, group_size, STATE_DEV)
    routed = lax.all_to_all(blocked, "states", split_axis=1, concat_axis=0, tiled=True)
    routed = routed.reshape(rows_here * group_size, STATE_DEV)
    owned_counts = jnp.sum(routed, axis=0, dtype=jnp.float32)
    piece = lax.all_gather(features, "states", axis=0, tiled=True)
    piece_f = piece.astype(jnp.float32)
    piece_sq = (piece_f * piece_f).astype(jnp.bfloat16)
    joined = jnp.concatenate([piece, piece_sq], axis=1)
    owned_sums = lax.dot_general(
        routed, joined, (((0,), (0,)), ((), ())), preferred_element_type=jnp.float32
    )
    mean_rows, prec_rows = refresh(
        owned_sums[:, :local_width], owned_sums[:, local_width:], owned_counts[:, None]
    )
    packed = lax.all_gather(
        jnp.concatenate([mean_rows, prec_rows], axis=1), "states", axis=0, tiled=True
    )
    means = packed[:, :local_width]
    precisions = packed[:, local_width:]
    mean_f = means.astype(jnp.float32)
    prec_f = precisions.astype(jnp.float32)
    product = (mean_f * prec_f).astype(jnp.bfloat16)
    constant_term = jnp.sum(mean_f * product.astype(jnp.float32) - jnp.log(prec_f), axis=1)
    lookup_table = jnp.concatenate([precisions, product], axis=1)
    weight_f = rounded.astype(jnp.float32)
    blended = jnp.dot(posterior, lookup_table, preferred_element_type=jnp.float32)
    quadratic = jnp.sum(
        squares.astype(jnp.float32) * blended[:, :local_width]
        - 2.0 * values * blended[:, local_width:],
        axis=1,
    )
    quadratic = quadratic + jnp.sum(weight_f * constant_term[state_ids], axis=1)
    summed = lax.psum(quadratic, "frames")
    weight_sum = jnp.sum(weight_f, axis=1)
    frame_score = -0.5 * summed / (full_width * weight_sum)
    return (means, precisions, frame_score)


def fits(mesh):
    return mesh.shape["states"] == 8 and mesh.shape["frames"] in (2, 4)


def solution(mesh):
    small = fits(mesh)
    return jax.shard_map(
        small_group if small else large_group,
        mesh=mesh,
        in_specs=(P("states", "frames"), P("states", None), P("states", None)),
        out_specs=(P(None, "frames"), P(None, "frames"), P("states")),
        check_vma=False,
    )
```

```python
import functools
import jax
import jax.numpy as jnp
from jax import lax
from jax.experimental import pallas as pl
from jax.experimental.pallas import tpu as pltpu
from jax.sharding import PartitionSpec as P


STATE_DEV = 96
GROUP = 128
PARTS = 4
variance_floor = 0.25
FAR = (4, 2, 7)


def vmem(n):
    return [pl.BlockSpec(memory_space=pltpu.VMEM)] * n


def swap(value, axis, k):
    n = lax.axis_size(axis)
    return lax.ppermute(value, axis, [(i, i ^ k) for i in range(n)])


def core():
    return lax.axis_index("states") % 2


def prep_kernel(feat_ref, ids_ref, wts_ref, msg_ref, ids_buf, wts_buf, sem):
    rows = feat_ref.shape[0]
    topk = ids_ref.shape[0]
    copies = [
        pltpu.make_async_copy(ids_ref, ids_buf, sem.at[0]),
        pltpu.make_async_copy(wts_ref, wts_buf, sem.at[1]),
    ]
    step = rows // PARTS
    for i in range(PARTS):
        part = pl.ds(i * step, step)
        copies.append(pltpu.make_async_copy(feat_ref.at[part], msg_ref.at[part], sem.at[2 + i]))
    for copy in copies:
        copy.start()
    copies[0].wait()
    ids = ids_buf[...]
    codes = (GROUP + (ids & (GROUP - 1))) << (ids >> 7)
    msg_ref[rows + topk :] = codes.astype(jnp.float32).astype(jnp.bfloat16)
    copies[1].wait()
    msg_ref[rows : rows + topk] = wts_buf[...].astype(jnp.bfloat16)
    for copy in copies[2:]:
        copy.wait()


def prep(features, ids, weights):
    rows, width = features.shape
    topk = ids.shape[0]
    return pl.pallas_call(
        prep_kernel,
        out_shape=jax.ShapeDtypeStruct((rows + 2 * topk, width), jnp.bfloat16),
        in_specs=[pl.BlockSpec(memory_space=pltpu.HBM)] * 3,
        out_specs=vmem(1)[0],
        scratch_shapes=[
            pltpu.VMEM(ids.shape, ids.dtype),
            pltpu.VMEM(weights.shape, weights.dtype),
            pltpu.SemaphoreType.DMA((2 + PARTS,)),
        ],
        compiler_params=pltpu.CompilerParams(vmem_limit_bytes=4 << 20),
        name="prep",
    )(*[pltpu.with_memory_space_constraint(v, pltpu.HBM) for v in (features, ids, weights)])


def build(ref, topk, post_ref, at, occ):
    width = ref.shape[1]
    rows = ref.shape[0] - 2 * topk
    states = post_ref.shape[0]
    groups = states // GROUP
    scale = (1 << (core() * groups)).astype(jnp.float32)
    base = (lax.broadcasted_iota(jnp.int32, (GROUP, 128), 0) + GROUP).astype(jnp.float32) * scale
    for tile in range(width // 128):
        lanes = slice(tile * 128, tile * 128 + 128)
        wts = ref[rows : rows + topk, lanes]
        codes = ref[rows + topk :, lanes]
        for group in range(groups):
            names = (base * float(2 ** group)).astype(jnp.bfloat16)
            acc = jnp.zeros((GROUP, 128), jnp.bfloat16)
            for j in range(topk):
                acc = jnp.where(codes[j : j + 1] == names, wts[j : j + 1], acc)
            post_ref[group * GROUP : (group + 1) * GROUP, at + tile * 128 : at + tile * 128 + 128] = acc
            part = acc.astype(jnp.float32)
            occ[group] = part if occ[group] is None else occ[group] + part


def fill(ref, topk, pair_ref, at):
    width = ref.shape[1]
    rows = ref.shape[0] - 2 * topk
    x = ref[:rows]
    pair_ref[at : at + rows, :width] = x
    pair_ref[at : at + rows, width:] = x * x


def gather_sums(msgs, topk, post_ref, pair_ref, old_sum, old_occ):
    width = msgs[0].shape[1]
    rows = msgs[0].shape[0] - 2 * topk
    groups = post_ref.shape[0] // GROUP
    occ = [None] * groups
    if old_occ is not None:
        occ = [old_occ[g * GROUP : (g + 1) * GROUP] for g in range(groups)]
    for i, ref in enumerate(msgs):
        build(ref, topk, post_ref, i * width, occ)
        fill(ref, topk, pair_ref, i * rows)
    total = jnp.dot(post_ref[...], pair_ref[...], preferred_element_type=jnp.float32)
    if old_sum is not None:
        total = total + old_sum[...]
    return total, occ


def moments_kernel(n, topk, first, *refs):
    msgs, rest = refs[:n], refs[n:]
    if first:
        sum_ref, occ_ref, post_ref, pair_ref = rest
        old_sum = old_occ = None
    else:
        old_sum, old_occ, sum_ref, occ_ref, post_ref, pair_ref = rest
    total, occ = gather_sums(msgs, topk, post_ref, pair_ref, old_sum, old_occ)
    sum_ref[...] = total
    for g, part in enumerate(occ):
        occ_ref[g * GROUP : (g + 1) * GROUP] = part


def moments(msgs, topk, states, old):
    width = msgs[0].shape[1]
    rows = msgs[0].shape[0] - 2 * topk
    n = len(msgs)
    first = not old
    post = jax.ShapeDtypeStruct((states, n * width), jnp.bfloat16)
    outs = [jax.ShapeDtypeStruct((states, 2 * width), jnp.float32), jax.ShapeDtypeStruct((states, 128), jnp.float32)]
    pair = jax.ShapeDtypeStruct((n * rows, 2 * width), jnp.bfloat16)
    scratch = []
    if first:
        outs += [post, pair]
    else:
        scratch = [pltpu.VMEM(v.shape, v.dtype) for v in (post, pair)]
    return pl.pallas_call(
        functools.partial(moments_kernel, n, topk, first),
        out_shape=tuple(outs),
        in_specs=vmem(n + len(old)),
        out_specs=tuple(vmem(len(outs))),
        scratch_shapes=scratch,
        compiler_params=pltpu.CompilerParams(vmem_limit_bytes=16 << 20),
        cost_estimate=pl.CostEstimate(flops=states * rows * n * 4000, bytes_accessed=1 << 20, transcendentals=0),
    )(*msgs, *old)


def final_kernel(n, topk, full_width, *refs):
    msgs = refs[:n]
    own_ref, near_ref, own_post_ref, both_ref, old_sum, old_occ = refs[n : n + 6]
    half_ref, score_ref, post_ref, pair_ref, table_ref = refs[n + 6 :]
    width = own_ref.shape[1]
    rows = own_ref.shape[0] - 2 * topk
    states = post_ref.shape[0]
    me = core()
    total, occ = gather_sums(msgs, topk, post_ref, pair_ref, old_sum, old_occ)
    occ = jnp.concatenate(occ, axis=0)
    inverse = 1.0 / jnp.sum(occ, axis=1, keepdims=True)
    mean = total[:, :width] * inverse
    variance = jnp.maximum(total[:, width:] * inverse - mean * mean, variance_floor)
    means = mean.astype(jnp.bfloat16)
    precs = (1.0 / variance).astype(jnp.bfloat16)
    half_ref[:states] = means
    half_ref[states:] = precs
    mean_f = means.astype(jnp.float32)
    prec_f = precs.astype(jnp.float32)
    product = (mean_f * prec_f).astype(jnp.bfloat16)
    constant = jnp.sum(mean_f * product.astype(jnp.float32) - jnp.log(prec_f), axis=1, keepdims=True)
    table_ref[:, :width] = product * jnp.bfloat16(-2.0)
    table_ref[:, width:] = precs
    likely = lax.dot_general(table_ref[...], both_ref[...], (((1,), (1,)), ((), ())), preferred_element_type=jnp.float32)
    quad = jnp.sum((likely + constant) * own_post_ref[...].astype(jnp.float32), axis=0, keepdims=True)
    for ref, row, at in ((own_ref, me, 0), (near_ref, 1 - me, rows)):
        wsum = jnp.sum(ref[rows : rows + topk].astype(jnp.float32), axis=0, keepdims=True)
        score_ref[pl.ds(row, 1)] = -0.5 * quad[:, at : at + rows] / (full_width * wsum)


def final(msgs, topk, own, near, own_post, both, old, full_width):
    width = own.shape[1]
    rows = own.shape[0] - 2 * topk
    states = own_post.shape[0]
    n = len(msgs)
    out = jax.ShapeDtypeStruct((2 * states, width), jnp.bfloat16)
    return pl.pallas_call(
        functools.partial(final_kernel, n, topk, float(full_width)),
        out_shape=(out, jax.ShapeDtypeStruct((2, rows), jnp.float32)),
        in_specs=vmem(n + 6),
        out_specs=tuple(vmem(2)),
        scratch_shapes=[
            pltpu.VMEM((states, n * width), jnp.bfloat16),
            pltpu.VMEM((n * rows, 2 * width), jnp.bfloat16),
            pltpu.VMEM((states, 2 * width), jnp.bfloat16),
        ],
        compiler_params=pltpu.CompilerParams(vmem_limit_bytes=16 << 20),
        cost_estimate=pl.CostEstimate(flops=8 * states * rows * 4 * width, bytes_accessed=4 << 20, transcendentals=0),
        name="final",
    )(*msgs, own, near, own_post, both, *old)


def place_kernel(mine_ref, other_ref, mean_out, prec_out, sem):
    states = mine_ref.shape[0] // 2
    copies = []
    for i, (ref, where) in enumerate(((mine_ref, core()), (other_ref, 1 - core()))):
        rows = pl.ds(pl.multiple_of(where * states, states), states)
        copies.append(pltpu.make_async_copy(ref.at[:states], mean_out.at[rows], sem.at[2 * i]))
        copies.append(pltpu.make_async_copy(ref.at[states:], prec_out.at[rows], sem.at[2 * i + 1]))
    for copy in copies:
        copy.start()
    for copy in copies:
        copy.wait()


def place(mine, other):
    hbm = pl.BlockSpec(memory_space=pltpu.HBM)
    out = jax.ShapeDtypeStruct(mine.shape, mine.dtype)
    return pl.pallas_call(
        place_kernel,
        out_shape=(out, out),
        in_specs=vmem(2),
        out_specs=(hbm, hbm),
        scratch_shapes=[pltpu.SemaphoreType.DMA((4,))],
        compiler_params=pltpu.CompilerParams(vmem_limit_bytes=4 << 20),
        cost_estimate=pl.CostEstimate(flops=1 << 20, bytes_accessed=1 << 20, transcendentals=0),
        name="place",
    )(mine, other)


def hop(value, pairs):
    return lax.ppermute(value, ("frames", "states"), pairs)


def small_group(features, state_ids, weights):
    return update(features, state_ids, weights)


def update(features, state_ids, weights):
    _, width = features.shape
    topk = state_ids.shape[1]
    group = lax.axis_size("states")
    depth = lax.axis_size("frames")
    states = STATE_DEV * group // 2
    own = prep(features, state_ids.T, weights.T)
    far = [swap(own, "states", k) for k in FAR]
    near = swap(own, "states", 1)
    back = [swap(v, "states", 1) for v in far]
    total, occ, post, both = moments([own, near], topk, states, ())
    old = moments([far[0]], topk, states, (total, occ))
    old = moments([back[0]], topk, states, old)
    old = moments([far[1]], topk, states, old)
    old = moments([back[1], far[2]], topk, states, old)
    half, score = final([back[2]], topk, own, near, post, both, old, width * depth)
    score = score + swap(score, "states", 1)
    other = swap(half, "states", 1)
    k = 1
    while k < depth:
        pairs = [(z * group + s, (z ^ k) * group + (s ^ 1)) for z in range(depth) for s in range(group)]
        score = score + hop(score, pairs)
        k *= 2
    means, precisions = place(half, other)
    return means, precisions, jnp.where(core() == 1, score[1], score[0])


def refresh(first, second, counts):
    mean_value = first / counts
    variance = jnp.maximum(second / counts - mean_value * mean_value, variance_floor)
    return (mean_value.astype(jnp.bfloat16), (1.0 / variance).astype(jnp.bfloat16))


def large_group(features, state_ids, weights):
    rows_here, local_width = features.shape
    group_size = lax.axis_size("states")
    full_width = local_width * lax.axis_size("frames")
    total_states = STATE_DEV * group_size
    row_index = jnp.arange(rows_here, dtype=jnp.int32)[:, None]
    rounded = weights.astype(jnp.bfloat16)
    posterior = (
        jnp.zeros((rows_here, total_states), jnp.bfloat16).at[row_index, state_ids].add(rounded)
    )
    values = features.astype(jnp.float32)
    squares = (values * values).astype(jnp.bfloat16)
    blocked = posterior.reshape(rows_here, group_size, STATE_DEV)
    routed = lax.all_to_all(blocked, "states", split_axis=1, concat_axis=0, tiled=True)
    routed = routed.reshape(rows_here * group_size, STATE_DEV)
    owned_counts = jnp.sum(routed, axis=0, dtype=jnp.float32)
    piece = lax.all_gather(features, "states", axis=0, tiled=True)
    piece_f = piece.astype(jnp.float32)
    piece_sq = (piece_f * piece_f).astype(jnp.bfloat16)
    joined = jnp.concatenate([piece, piece_sq], axis=1)
    owned_sums = lax.dot_general(
        routed, joined, (((0,), (0,)), ((), ())), preferred_element_type=jnp.float32
    )
    mean_rows, prec_rows = refresh(
        owned_sums[:, :local_width], owned_sums[:, local_width:], owned_counts[:, None]
    )
    packed = lax.all_gather(
        jnp.concatenate([mean_rows, prec_rows], axis=1), "states", axis=0, tiled=True
    )
    means = packed[:, :local_width]
    precisions = packed[:, local_width:]
    mean_f = means.astype(jnp.float32)
    prec_f = precisions.astype(jnp.float32)
    product = (mean_f * prec_f).astype(jnp.bfloat16)
    constant_term = jnp.sum(mean_f * product.astype(jnp.float32) - jnp.log(prec_f), axis=1)
    lookup_table = jnp.concatenate([precisions, product], axis=1)
    weight_f = rounded.astype(jnp.float32)
    blended = jnp.dot(posterior, lookup_table, preferred_element_type=jnp.float32)
    quadratic = jnp.sum(
        squares.astype(jnp.float32) * blended[:, :local_width]
        - 2.0 * values * blended[:, local_width:],
        axis=1,
    )
    quadratic = quadratic + jnp.sum(weight_f * constant_term[state_ids], axis=1)
    summed = lax.psum(quadratic, "frames")
    weight_sum = jnp.sum(weight_f, axis=1)
    frame_score = -0.5 * summed / (full_width * weight_sum)
    return (means, precisions, frame_score)


def fits(mesh):
    return mesh.shape["states"] == 8 and mesh.shape["frames"] in (2, 4)


def solution(mesh):
    small = fits(mesh)
    return jax.shard_map(
        small_group if small else large_group,
        mesh=mesh,
        in_specs=(P("states", "frames"), P("states", None), P("states", None)),
        out_specs=(P(None, "frames"), P(None, "frames"), P("states")),
        check_vma=False,
    )
```

```python
import functools
import jax
import jax.numpy as jnp
from jax import lax
from jax.experimental import pallas as pl
from jax.experimental.pallas import tpu as pltpu
from jax.sharding import PartitionSpec as P


STATE_DEV = 96
GROUP = 128
PARTS = 4
variance_floor = 0.25
FAR = (4, 2, 7)


def vmem(n):
    return [pl.BlockSpec(memory_space=pltpu.VMEM)] * n


def swap(value, axis, k):
    n = lax.axis_size(axis)
    return lax.ppermute(value, axis, [(i, i ^ k) for i in range(n)])


def core():
    return lax.axis_index("states") % 2


def prep_kernel(feat_ref, ids_ref, wts_ref, msg_ref, ids_buf, wts_buf, sem):
    rows = feat_ref.shape[0]
    topk = ids_ref.shape[0]
    copies = [
        pltpu.make_async_copy(ids_ref, ids_buf, sem.at[0]),
        pltpu.make_async_copy(wts_ref, wts_buf, sem.at[1]),
    ]
    step = rows // PARTS
    for i in range(PARTS):
        part = pl.ds(i * step, step)
        copies.append(pltpu.make_async_copy(feat_ref.at[part], msg_ref.at[part], sem.at[2 + i]))
    for copy in copies:
        copy.start()
    copies[0].wait()
    ids = ids_buf[...]
    codes = (GROUP + (ids & (GROUP - 1))) << (ids >> 7)
    msg_ref[rows + topk :] = codes.astype(jnp.float32).astype(jnp.bfloat16)
    copies[1].wait()
    msg_ref[rows : rows + topk] = wts_buf[...].astype(jnp.bfloat16)
    for copy in copies[2:]:
        copy.wait()


def prep(features, ids, weights):
    rows, width = features.shape
    topk = ids.shape[0]
    return pl.pallas_call(
        prep_kernel,
        out_shape=jax.ShapeDtypeStruct((rows + 2 * topk, width), jnp.bfloat16),
        in_specs=[pl.BlockSpec(memory_space=pltpu.HBM)] * 3,
        out_specs=vmem(1)[0],
        scratch_shapes=[
            pltpu.VMEM(ids.shape, ids.dtype),
            pltpu.VMEM(weights.shape, weights.dtype),
            pltpu.SemaphoreType.DMA((2 + PARTS,)),
        ],
        compiler_params=pltpu.CompilerParams(vmem_limit_bytes=4 << 20),
        name="prep",
    )(*[pltpu.with_memory_space_constraint(v, pltpu.HBM) for v in (features, ids, weights)])


def build(ref, topk, post_ref, at, occ):
    width = ref.shape[1]
    rows = ref.shape[0] - 2 * topk
    states = post_ref.shape[0]
    groups = states // GROUP
    scale = (1 << (core() * groups)).astype(jnp.float32)
    base = (lax.broadcasted_iota(jnp.int32, (GROUP, 128), 0) + GROUP).astype(jnp.float32) * scale
    for tile in range(width // 128):
        lanes = slice(tile * 128, tile * 128 + 128)
        wts = ref[rows : rows + topk, lanes]
        codes = ref[rows + topk :, lanes]
        for group in range(groups):
            names = (base * float(2 ** group)).astype(jnp.bfloat16)
            acc = jnp.zeros((GROUP, 128), jnp.bfloat16)
            for j in range(topk):
                acc = jnp.where(codes[j : j + 1] == names, wts[j : j + 1], acc)
            post_ref[group * GROUP : (group + 1) * GROUP, at + tile * 128 : at + tile * 128 + 128] = acc
            part = acc.astype(jnp.float32)
            occ[group] = part if occ[group] is None else occ[group] + part


def fill(ref, topk, pair_ref, at):
    width = ref.shape[1]
    rows = ref.shape[0] - 2 * topk
    x = ref[:rows]
    pair_ref[at : at + rows, :width] = x
    pair_ref[at : at + rows, width:] = x * x


def gather_sums(msgs, topk, post_ref, pair_ref, old_sum, old_occ):
    width = msgs[0].shape[1]
    rows = msgs[0].shape[0] - 2 * topk
    groups = post_ref.shape[0] // GROUP
    occ = [None] * groups
    if old_occ is not None:
        occ = [old_occ[g * GROUP : (g + 1) * GROUP] for g in range(groups)]
    for i, ref in enumerate(msgs):
        build(ref, topk, post_ref, i * width, occ)
        fill(ref, topk, pair_ref, i * rows)
    total = jnp.dot(post_ref[...], pair_ref[...], preferred_element_type=jnp.float32)
    if old_sum is not None:
        total = total + old_sum[...]
    return total, occ


def moments_kernel(n, topk, first, *refs):
    msgs, rest = refs[:n], refs[n:]
    if first:
        sum_ref, occ_ref, post_ref, pair_ref = rest
        old_sum = old_occ = None
    else:
        old_sum, old_occ, sum_ref, occ_ref, post_ref, pair_ref = rest
    total, occ = gather_sums(msgs, topk, post_ref, pair_ref, old_sum, old_occ)
    sum_ref[...] = total
    for g, part in enumerate(occ):
        occ_ref[g * GROUP : (g + 1) * GROUP] = part


def moments(msgs, topk, states, old):
    width = msgs[0].shape[1]
    rows = msgs[0].shape[0] - 2 * topk
    n = len(msgs)
    first = not old
    post = jax.ShapeDtypeStruct((states, n * width), jnp.bfloat16)
    outs = [jax.ShapeDtypeStruct((states, 2 * width), jnp.float32), jax.ShapeDtypeStruct((states, 128), jnp.float32)]
    pair = jax.ShapeDtypeStruct((n * rows, 2 * width), jnp.bfloat16)
    scratch = []
    if first:
        outs += [post, pair]
    else:
        scratch = [pltpu.VMEM(v.shape, v.dtype) for v in (post, pair)]
    return pl.pallas_call(
        functools.partial(moments_kernel, n, topk, first),
        out_shape=tuple(outs),
        in_specs=vmem(n + len(old)),
        out_specs=tuple(vmem(len(outs))),
        scratch_shapes=scratch,
        compiler_params=pltpu.CompilerParams(vmem_limit_bytes=16 << 20),
        cost_estimate=pl.CostEstimate(flops=states * rows * n * 4000, bytes_accessed=1 << 20, transcendentals=0),
    )(*msgs, *old)


def final_kernel(n, topk, full_width, *refs):
    msgs = refs[:n]
    own_ref, near_ref, own_post_ref, both_ref, old_sum, old_occ = refs[n : n + 6]
    half_ref, score_ref, post_ref, pair_ref, table_ref = refs[n + 6 :]
    width = own_ref.shape[1]
    rows = own_ref.shape[0] - 2 * topk
    states = post_ref.shape[0]
    me = core()
    total, occ = gather_sums(msgs, topk, post_ref, pair_ref, old_sum, old_occ)
    occ = jnp.concatenate(occ, axis=0)
    inverse = 1.0 / jnp.sum(occ, axis=1, keepdims=True)
    mean = total[:, :width] * inverse
    variance = jnp.maximum(total[:, width:] * inverse - mean * mean, variance_floor)
    means = mean.astype(jnp.bfloat16)
    precs = (1.0 / variance).astype(jnp.bfloat16)
    half_ref[:states] = means
    half_ref[states:] = precs
    mean_f = means.astype(jnp.float32)
    prec_f = precs.astype(jnp.float32)
    product = (mean_f * prec_f).astype(jnp.bfloat16)
    constant = jnp.sum(mean_f * product.astype(jnp.float32) - jnp.log(prec_f), axis=1, keepdims=True)
    table_ref[:, :width] = product * jnp.bfloat16(-2.0)
    table_ref[:, width:] = precs
    likely = lax.dot_general(table_ref[...], both_ref[...], (((1,), (1,)), ((), ())), preferred_element_type=jnp.float32)
    quad = jnp.sum((likely + constant) * own_post_ref[...].astype(jnp.float32), axis=0, keepdims=True)
    for ref, row, at in ((own_ref, me, 0), (near_ref, 1 - me, rows)):
        wsum = jnp.sum(ref[rows : rows + topk].astype(jnp.float32), axis=0, keepdims=True)
        score_ref[pl.ds(row, 1)] = -0.5 * quad[:, at : at + rows] / (full_width * wsum)


def final(msgs, topk, own, near, own_post, both, old, full_width):
    width = own.shape[1]
    rows = own.shape[0] - 2 * topk
    states = own_post.shape[0]
    n = len(msgs)
    out = jax.ShapeDtypeStruct((2 * states, width), jnp.bfloat16)
    return pl.pallas_call(
        functools.partial(final_kernel, n, topk, float(full_width)),
        out_shape=(out, jax.ShapeDtypeStruct((2, rows), jnp.float32)),
        in_specs=vmem(n + 6),
        out_specs=tuple(vmem(2)),
        scratch_shapes=[
            pltpu.VMEM((states, n * width), jnp.bfloat16),
            pltpu.VMEM((n * rows, 2 * width), jnp.bfloat16),
            pltpu.VMEM((states, 2 * width), jnp.bfloat16),
        ],
        compiler_params=pltpu.CompilerParams(vmem_limit_bytes=16 << 20),
        cost_estimate=pl.CostEstimate(flops=8 * states * rows * 4 * width, bytes_accessed=4 << 20, transcendentals=0),
        name="final",
    )(*msgs, own, near, own_post, both, *old)


def place_kernel(mine_ref, other_ref, mean_out, prec_out, sem):
    states = mine_ref.shape[0] // 2
    copies = []
    for i, (ref, where) in enumerate(((mine_ref, core()), (other_ref, 1 - core()))):
        rows = pl.ds(pl.multiple_of(where * states, states), states)
        copies.append(pltpu.make_async_copy(ref.at[:states], mean_out.at[rows], sem.at[2 * i]))
        copies.append(pltpu.make_async_copy(ref.at[states:], prec_out.at[rows], sem.at[2 * i + 1]))
    for copy in copies:
        copy.start()
    for copy in copies:
        copy.wait()


def place(mine, other):
    hbm = pl.BlockSpec(memory_space=pltpu.HBM)
    out = jax.ShapeDtypeStruct(mine.shape, mine.dtype)
    return pl.pallas_call(
        place_kernel,
        out_shape=(out, out),
        in_specs=vmem(2),
        out_specs=(hbm, hbm),
        scratch_shapes=[pltpu.SemaphoreType.DMA((4,))],
        compiler_params=pltpu.CompilerParams(vmem_limit_bytes=4 << 20),
        cost_estimate=pl.CostEstimate(flops=1 << 20, bytes_accessed=1 << 20, transcendentals=0),
        name="place",
    )(mine, other)


def hop(value, pairs):
    return lax.ppermute(value, ("frames", "states"), pairs)


def small_group(features, state_ids, weights):
    return update(features, state_ids, weights)


def update(features, state_ids, weights):
    _, width = features.shape
    topk = state_ids.shape[1]
    group = lax.axis_size("states")
    depth = lax.axis_size("frames")
    states = STATE_DEV * group // 2
    own = prep(features, state_ids.T, weights.T)
    far = [swap(own, "states", k) for k in FAR]
    near = swap(own, "states", 1)
    back = [swap(v, "states", 1) for v in far]
    total, occ, post, both = moments([own, near], topk, states, ())
    old = moments([far[0]], topk, states, (total, occ))
    old = moments([back[0]], topk, states, old)
    old = moments([far[1]], topk, states, old)
    old = moments([back[1], far[2]], topk, states, old)
    half, score = final([back[2]], topk, own, near, post, both, old, width * depth)
    score = score + swap(score, "states", 1)
    other = swap(half, "states", 1)
    k = 1
    while k < depth:
        pairs = [(z * group + s, (z ^ k) * group + (s ^ 1)) for z in range(depth) for s in range(group)]
        score = score + hop(score, pairs)
        k *= 2
    means, precisions = place(half, other)
    return means, precisions, jnp.where(core() == 1, score[1], score[0])


def refresh(first, second, counts):
    mean_value = first / counts
    variance = jnp.maximum(second / counts - mean_value * mean_value, variance_floor)
    return (mean_value.astype(jnp.bfloat16), (1.0 / variance).astype(jnp.bfloat16))


def large_group(features, state_ids, weights):
    rows_here, local_width = features.shape
    group_size = lax.axis_size("states")
    full_width = local_width * lax.axis_size("frames")
    total_states = STATE_DEV * group_size
    rounded = lax.optimization_barrier(weights.astype(jnp.bfloat16))
    names = jnp.arange(total_states, dtype=jnp.int32)

    def step(j, posterior):
        chosen = lax.dynamic_slice_in_dim(state_ids, j, 1, axis=1)
        value = lax.dynamic_slice_in_dim(rounded, j, 1, axis=1)
        return jnp.where(chosen == names[None, :], value, posterior)

    posterior = lax.fori_loop(
        0, state_ids.shape[1], step, jnp.zeros((rows_here, total_states), jnp.bfloat16), unroll=8
    )
    values = features.astype(jnp.float32)
    squares = (values * values).astype(jnp.bfloat16)
    blocked = posterior.reshape(rows_here, group_size, STATE_DEV)
    routed = lax.all_to_all(blocked, "states", split_axis=1, concat_axis=0, tiled=True)
    routed = routed.reshape(rows_here * group_size, STATE_DEV)
    owned_counts = jnp.sum(routed, axis=0, dtype=jnp.float32)
    piece = lax.all_gather(features, "states", axis=0, tiled=True)
    piece_f = piece.astype(jnp.float32)
    piece_sq = (piece_f * piece_f).astype(jnp.bfloat16)
    joined = jnp.concatenate([piece, piece_sq], axis=1)
    owned_sums = lax.dot_general(
        routed, joined, (((0,), (0,)), ((), ())), preferred_element_type=jnp.float32
    )
    mean_rows, prec_rows = refresh(
        owned_sums[:, :local_width], owned_sums[:, local_width:], owned_counts[:, None]
    )
    packed = lax.all_gather(
        jnp.concatenate([mean_rows, prec_rows], axis=1), "states", axis=0, tiled=True
    )
    means = packed[:, :local_width]
    precisions = packed[:, local_width:]
    mean_f = means.astype(jnp.float32)
    prec_f = precisions.astype(jnp.float32)
    product = (mean_f * prec_f).astype(jnp.bfloat16)
    constant_term = jnp.sum(mean_f * product.astype(jnp.float32) - jnp.log(prec_f), axis=1)
    lookup_table = jnp.concatenate([precisions, product * jnp.bfloat16(-2.0)], axis=1)
    both = jnp.concatenate([squares, features], axis=1)
    likely = lax.dot_general(both, lookup_table, (((1,), (1,)), ((), ())), preferred_element_type=jnp.float32)
    quadratic = jnp.sum((likely + constant_term[None, :]) * posterior.astype(jnp.float32), axis=1)
    weight_f = rounded.astype(jnp.float32)
    summed = lax.psum(quadratic, "frames")
    weight_sum = jnp.sum(weight_f, axis=1)
    frame_score = -0.5 * summed / (full_width * weight_sum)
    return (means, precisions, frame_score)


def fits(mesh):
    return mesh.shape["states"] == 8 and mesh.shape["frames"] in (2, 4)


def solution(mesh):
    small = fits(mesh)
    return jax.shard_map(
        small_group if small else large_group,
        mesh=mesh,
        in_specs=(P("states", "frames"), P("states", None), P("states", None)),
        out_specs=(P(None, "frames"), P(None, "frames"), P("states")),
        check_vma=False,
    )
```

```python
import functools
import jax
import jax.numpy as jnp
from jax import lax
from jax.experimental import pallas as pl
from jax.experimental.pallas import tpu as pltpu
from jax.sharding import PartitionSpec as P


STATE_DEV = 96
GROUP = 128
PARTS = 4
variance_floor = 0.25
FAR = (4, 2, 7)


def vmem(n):
    return [pl.BlockSpec(memory_space=pltpu.VMEM)] * n


def swap(value, axis, k):
    n = lax.axis_size(axis)
    return lax.ppermute(value, axis, [(i, i ^ k) for i in range(n)])


def core():
    return lax.axis_index("states") % 2


def prep_kernel(feat_ref, ids_ref, wts_ref, msg_ref, ids_buf, wts_buf, sem):
    rows = feat_ref.shape[0]
    topk = ids_ref.shape[0]
    copies = [
        pltpu.make_async_copy(ids_ref, ids_buf, sem.at[0]),
        pltpu.make_async_copy(wts_ref, wts_buf, sem.at[1]),
    ]
    step = rows // PARTS
    for i in range(PARTS):
        part = pl.ds(i * step, step)
        copies.append(pltpu.make_async_copy(feat_ref.at[part], msg_ref.at[part], sem.at[2 + i]))
    for copy in copies[2:] + copies[:2]:
        copy.start()
    copies[0].wait()
    ids = ids_buf[...]
    codes = (GROUP + (ids & (GROUP - 1))) << (ids >> 7)
    msg_ref[rows + topk :] = codes.astype(jnp.float32).astype(jnp.bfloat16)
    copies[1].wait()
    msg_ref[rows : rows + topk] = wts_buf[...].astype(jnp.bfloat16)
    for copy in copies[2:]:
        copy.wait()


def prep(features, ids, weights):
    rows, width = features.shape
    topk = ids.shape[0]
    return pl.pallas_call(
        prep_kernel,
        out_shape=jax.ShapeDtypeStruct((rows + 2 * topk, width), jnp.bfloat16),
        in_specs=[pl.BlockSpec(memory_space=pltpu.HBM)] * 3,
        out_specs=vmem(1)[0],
        scratch_shapes=[
            pltpu.VMEM(ids.shape, ids.dtype),
            pltpu.VMEM(weights.shape, weights.dtype),
            pltpu.SemaphoreType.DMA((2 + PARTS,)),
        ],
        compiler_params=pltpu.CompilerParams(vmem_limit_bytes=4 << 20),
        name="prep",
    )(*[pltpu.with_memory_space_constraint(v, pltpu.HBM) for v in (features, ids, weights)])


def build(ref, topk, post_ref, at, occ):
    width = ref.shape[1]
    rows = ref.shape[0] - 2 * topk
    states = post_ref.shape[0]
    groups = states // GROUP
    scale = (1 << (core() * groups)).astype(jnp.float32)
    base = (lax.broadcasted_iota(jnp.int32, (GROUP, 128), 0) + GROUP).astype(jnp.float32) * scale
    for tile in range(width // 128):
        lanes = slice(tile * 128, tile * 128 + 128)
        wts = ref[rows : rows + topk, lanes]
        codes = ref[rows + topk :, lanes]
        for group in range(groups):
            names = (base * float(2 ** group)).astype(jnp.bfloat16)
            acc = jnp.zeros((GROUP, 128), jnp.bfloat16)
            for j in range(topk):
                acc = jnp.where(codes[j : j + 1] == names, wts[j : j + 1], acc)
            post_ref[group * GROUP : (group + 1) * GROUP, at + tile * 128 : at + tile * 128 + 128] = acc
            part = acc.astype(jnp.float32)
            occ[group] = part if occ[group] is None else occ[group] + part


def fill(ref, topk, pair_ref, at):
    width = ref.shape[1]
    rows = ref.shape[0] - 2 * topk
    x = ref[:rows]
    pair_ref[at : at + rows, :width] = x
    pair_ref[at : at + rows, width:] = x * x


def gather_sums(msgs, topk, post_ref, pair_ref, old_sum, old_occ):
    width = msgs[0].shape[1]
    rows = msgs[0].shape[0] - 2 * topk
    groups = post_ref.shape[0] // GROUP
    occ = [None] * groups
    if old_occ is not None:
        occ = [old_occ[g * GROUP : (g + 1) * GROUP] for g in range(groups)]
    for i, ref in enumerate(msgs):
        build(ref, topk, post_ref, i * width, occ)
        fill(ref, topk, pair_ref, i * rows)
    total = jnp.dot(post_ref[...], pair_ref[...], preferred_element_type=jnp.float32)
    if old_sum is not None:
        total = total + old_sum[...]
    return total, occ


def moments_kernel(n, topk, first, *refs):
    msgs, rest = refs[:n], refs[n:]
    if first:
        sum_ref, occ_ref, post_ref, pair_ref = rest
        old_sum = old_occ = None
    else:
        old_sum, old_occ, sum_ref, occ_ref, post_ref, pair_ref = rest
    total, occ = gather_sums(msgs, topk, post_ref, pair_ref, old_sum, old_occ)
    sum_ref[...] = total
    for g, part in enumerate(occ):
        occ_ref[g * GROUP : (g + 1) * GROUP] = part


def moments(msgs, topk, states, old):
    width = msgs[0].shape[1]
    rows = msgs[0].shape[0] - 2 * topk
    n = len(msgs)
    first = not old
    post = jax.ShapeDtypeStruct((states, n * width), jnp.bfloat16)
    outs = [jax.ShapeDtypeStruct((states, 2 * width), jnp.float32), jax.ShapeDtypeStruct((states, 128), jnp.float32)]
    pair = jax.ShapeDtypeStruct((n * rows, 2 * width), jnp.bfloat16)
    scratch = []
    if first:
        outs += [post, pair]
    else:
        scratch = [pltpu.VMEM(v.shape, v.dtype) for v in (post, pair)]
    return pl.pallas_call(
        functools.partial(moments_kernel, n, topk, first),
        out_shape=tuple(outs),
        in_specs=vmem(n + len(old)),
        out_specs=tuple(vmem(len(outs))),
        scratch_shapes=scratch,
        compiler_params=pltpu.CompilerParams(vmem_limit_bytes=16 << 20),
        cost_estimate=pl.CostEstimate(flops=states * rows * n * 4000, bytes_accessed=1 << 20, transcendentals=0),
    )(*msgs, *old)


def final_kernel(n, topk, full_width, *refs):
    msgs = refs[:n]
    own_ref, near_ref, own_post_ref, both_ref, old_sum, old_occ = refs[n : n + 6]
    half_ref, score_ref, post_ref, pair_ref, table_ref = refs[n + 6 :]
    width = own_ref.shape[1]
    rows = own_ref.shape[0] - 2 * topk
    states = post_ref.shape[0]
    me = core()
    total, occ = gather_sums(msgs, topk, post_ref, pair_ref, old_sum, old_occ)
    occ = jnp.concatenate(occ, axis=0)
    inverse = 1.0 / jnp.sum(occ, axis=1, keepdims=True)
    mean = total[:, :width] * inverse
    variance = jnp.maximum(total[:, width:] * inverse - mean * mean, variance_floor)
    means = mean.astype(jnp.bfloat16)
    precs = (1.0 / variance).astype(jnp.bfloat16)
    half_ref[:states] = means
    half_ref[states:] = precs
    mean_f = means.astype(jnp.float32)
    prec_f = precs.astype(jnp.float32)
    product = means * precs
    half = width // 2
    paired = mean_f * product.astype(jnp.float32)
    logs = jnp.log(prec_f[:, :half] * prec_f[:, half:])
    constant = jnp.sum(paired[:, :half] + paired[:, half:] - logs, axis=1, keepdims=True)
    table_ref[:, :width] = product * jnp.bfloat16(-2.0)
    table_ref[:, width:] = precs
    likely = lax.dot_general(table_ref[...], both_ref[...], (((1,), (1,)), ((), ())), preferred_element_type=jnp.float32)
    quad = jnp.sum((likely + constant) * own_post_ref[...].astype(jnp.float32), axis=0, keepdims=True)
    for ref, row, at in ((own_ref, me, 0), (near_ref, 1 - me, rows)):
        wsum = jnp.sum(ref[rows : rows + topk].astype(jnp.float32), axis=0, keepdims=True)
        score_ref[pl.ds(row, 1)] = -0.5 * quad[:, at : at + rows] / (full_width * wsum)


def final(msgs, topk, own, near, own_post, both, old, full_width):
    width = own.shape[1]
    rows = own.shape[0] - 2 * topk
    states = own_post.shape[0]
    n = len(msgs)
    out = jax.ShapeDtypeStruct((2 * states, width), jnp.bfloat16)
    return pl.pallas_call(
        functools.partial(final_kernel, n, topk, float(full_width)),
        out_shape=(out, jax.ShapeDtypeStruct((2, rows), jnp.float32)),
        in_specs=vmem(n + 6),
        out_specs=tuple(vmem(2)),
        scratch_shapes=[
            pltpu.VMEM((states, n * width), jnp.bfloat16),
            pltpu.VMEM((n * rows, 2 * width), jnp.bfloat16),
            pltpu.VMEM((states, 2 * width), jnp.bfloat16),
        ],
        compiler_params=pltpu.CompilerParams(vmem_limit_bytes=16 << 20),
        cost_estimate=pl.CostEstimate(flops=8 * states * rows * 4 * width, bytes_accessed=4 << 20, transcendentals=0),
        name="final",
    )(*msgs, own, near, own_post, both, *old)


def place_kernel(mine_ref, other_ref, mean_out, prec_out, sem):
    states = mine_ref.shape[0] // 2
    copies = []
    for i, (ref, where) in enumerate(((mine_ref, core()), (other_ref, 1 - core()))):
        rows = pl.ds(pl.multiple_of(where * states, states), states)
        copies.append(pltpu.make_async_copy(ref.at[:states], mean_out.at[rows], sem.at[2 * i]))
        copies.append(pltpu.make_async_copy(ref.at[states:], prec_out.at[rows], sem.at[2 * i + 1]))
    for copy in copies:
        copy.start()
    for copy in copies:
        copy.wait()


def place(mine, other):
    hbm = pl.BlockSpec(memory_space=pltpu.HBM)
    out = jax.ShapeDtypeStruct(mine.shape, mine.dtype)
    return pl.pallas_call(
        place_kernel,
        out_shape=(out, out),
        in_specs=vmem(2),
        out_specs=(hbm, hbm),
        scratch_shapes=[pltpu.SemaphoreType.DMA((4,))],
        compiler_params=pltpu.CompilerParams(vmem_limit_bytes=4 << 20),
        cost_estimate=pl.CostEstimate(flops=1 << 20, bytes_accessed=1 << 20, transcendentals=0),
        name="place",
    )(mine, other)


def hop(value, pairs):
    return lax.ppermute(value, ("frames", "states"), pairs)


def small_group(features, state_ids, weights):
    return update(features, state_ids, weights)


def update(features, state_ids, weights):
    _, width = features.shape
    topk = state_ids.shape[1]
    group = lax.axis_size("states")
    depth = lax.axis_size("frames")
    states = STATE_DEV * group // 2
    own = prep(features, state_ids.T, weights.T)
    far = [swap(own, "states", k) for k in FAR]
    near = swap(own, "states", 1)
    back = [swap(v, "states", 1) for v in far]
    total, occ, post, both = moments([own, near], topk, states, ())
    old = moments([far[0], back[0]], topk, states, (total, occ))
    old = moments([far[1]], topk, states, old)
    old = moments([back[1], far[2]], topk, states, old)
    half, score = final([back[2]], topk, own, near, post, both, old, width * depth)
    score = score + swap(score, "states", 1)
    other = swap(half, "states", 1)
    k = 1
    while k < depth:
        pairs = [(z * group + s, (z ^ k) * group + (s ^ 1)) for z in range(depth) for s in range(group)]
        score = score + hop(score, pairs)
        k *= 2
    means, precisions = place(half, other)
    return means, precisions, jnp.where(core() == 1, score[1], score[0])


def refresh(first, second, counts):
    mean_value = first / counts
    variance = jnp.maximum(second / counts - mean_value * mean_value, variance_floor)
    return (mean_value.astype(jnp.bfloat16), (1.0 / variance).astype(jnp.bfloat16))


def large_group(features, state_ids, weights):
    rows_here, local_width = features.shape
    group_size = lax.axis_size("states")
    full_width = local_width * lax.axis_size("frames")
    total_states = STATE_DEV * group_size
    rounded = lax.optimization_barrier(weights.astype(jnp.bfloat16))
    names = jnp.arange(total_states, dtype=jnp.int32)

    def step(j, posterior):
        chosen = lax.dynamic_slice_in_dim(state_ids, j, 1, axis=1)
        value = lax.dynamic_slice_in_dim(rounded, j, 1, axis=1)
        return jnp.where(chosen == names[None, :], value, posterior)

    posterior = lax.fori_loop(
        0, state_ids.shape[1], step, jnp.zeros((rows_here, total_states), jnp.bfloat16), unroll=8
    )
    values = features.astype(jnp.float32)
    squares = (values * values).astype(jnp.bfloat16)
    blocked = posterior.reshape(rows_here, group_size, STATE_DEV)
    routed = lax.all_to_all(blocked, "states", split_axis=1, concat_axis=0, tiled=True)
    routed = routed.reshape(rows_here * group_size, STATE_DEV)
    owned_counts = jnp.sum(routed, axis=0, dtype=jnp.float32)
    piece = lax.all_gather(features, "states", axis=0, tiled=True)
    piece_f = piece.astype(jnp.float32)
    piece_sq = (piece_f * piece_f).astype(jnp.bfloat16)
    joined = jnp.concatenate([piece, piece_sq], axis=1)
    owned_sums = lax.dot_general(
        routed, joined, (((0,), (0,)), ((), ())), preferred_element_type=jnp.float32
    )
    mean_rows, prec_rows = refresh(
        owned_sums[:, :local_width], owned_sums[:, local_width:], owned_counts[:, None]
    )
    packed = lax.all_gather(
        jnp.concatenate([mean_rows, prec_rows], axis=1), "states", axis=0, tiled=True
    )
    means = packed[:, :local_width]
    precisions = packed[:, local_width:]
    mean_f = means.astype(jnp.float32)
    prec_f = precisions.astype(jnp.float32)
    product = (mean_f * prec_f).astype(jnp.bfloat16)
    constant_term = jnp.sum(mean_f * product.astype(jnp.float32) - jnp.log(prec_f), axis=1)
    lookup_table = jnp.concatenate([precisions, product * jnp.bfloat16(-2.0)], axis=1)
    both = jnp.concatenate([squares, features], axis=1)
    likely = lax.dot_general(both, lookup_table, (((1,), (1,)), ((), ())), preferred_element_type=jnp.float32)
    quadratic = jnp.sum((likely + constant_term[None, :]) * posterior.astype(jnp.float32), axis=1)
    weight_f = rounded.astype(jnp.float32)
    summed = lax.psum(quadratic, "frames")
    weight_sum = jnp.sum(weight_f, axis=1)
    frame_score = -0.5 * summed / (full_width * weight_sum)
    return (means, precisions, frame_score)


def fits(mesh):
    return mesh.shape["states"] == 8 and mesh.shape["frames"] in (2, 4)


def solution(mesh):
    small = fits(mesh)
    return jax.shard_map(
        small_group if small else large_group,
        mesh=mesh,
        in_specs=(P("states", "frames"), P("states", None), P("states", None)),
        out_specs=(P(None, "frames"), P(None, "frames"), P("states")),
        check_vma=False,
    )
```
